32 devices in a mesh: inter: 4 (over y, x), intra: 8 (over z, core).
Axes of the slice: x: 2, y: 2, z: 4, core: 2. Of those that a mesh axis runs over, the one named last changes fastest.
Arguments:
- layer_input: bfloat16 [4096, 4608], P(('inter', 'intra')), may hold values from -80 to 80
- norm_gain: bfloat16 [4608], P('intra'), may hold values from 0.5 to 1.5
- kv_weight: bfloat16 [4608, 128], P('intra'), may hold values from -0.09375 to 0.09375
- kv_cotangent: bfloat16 [4096, 128], P(('inter', 'intra')), may hold values from -24 to 24
Outputs:
- input_grad: bfloat16 [4096, 4608], P(('inter', 'intra'))
- weight_grad: float32 [4608, 128], P(('inter', 'intra'))
- gain_grad: float32 [4608], P(('inter', 'intra'))
The draws below stay inside these ranges and needn't reach their ends.
All inputs are finite; a program needn't handle non-finite values.
Results may differ from the reference program's by a relative error of at most 0.0029.
Values may be sent and summed in bfloat16 or wider, within the bound.
A program may use at most 64 MiB of HBM per device.

```python
import math
import jax
import jax.numpy as jnp
from jax import lax

D = 4608
HD = 64
TOK_DEV = 128
TOKENS = 4096
N_INTER = 4
N_INTRA = 8


def draw_layer_input(key, part):
    key_base = jax.random.fold_in(key, 11)
    key_rows = jax.random.fold_in(key, 12)
    key_cols = jax.random.fold_in(key, 13)
    values = jnp.clip(jax.random.normal(key_base, (TOKENS, D), jnp.float32), -4.0, 4.0)
    lowest = 0.3
    highest = 3.0
    row_scale = jnp.exp(jax.random.uniform(key_rows, (TOKENS, 1), jnp.float32, math.log(lowest), math.log(highest)))
    col_scale = jnp.exp(jax.random.uniform(key_cols, (1, D), jnp.float32, math.log(lowest), math.log(highest)))
    return (values * row_scale * col_scale).astype(jnp.bfloat16)


def block_levels(rng, dims, cuts, least, high):
    def one(position, parts):
        draws = jax.random.uniform(jax.random.fold_in(jax.random.fold_in(rng, 6), position), (parts,), jnp.float32, least / len(cuts), high / len(cuts))
        return jnp.repeat(jnp.exp(draws), dims[position] // parts).reshape((-1,) + (1,) * (len(dims) - position - 1))

    factor_of = one(*cuts[0])
    for cut in cuts[1:]:
        factor_of = factor_of * one(*cut)
    return factor_of


def centred(key, dims, spread, bound, cuts=(), kind=jnp.bfloat16):
    loudness = block_levels(key, dims, cuts, -0.22, 0.18) if cuts else 1.0
    values = jax.random.normal(key, dims, jnp.float32) * spread * loudness
    return jnp.minimum(jnp.maximum(values, -bound), bound).astype(kind)


def setup_inputs(seed: int = 0) -> dict:
    key_list = jax.random.split(jax.random.key(seed), 5)
    layer_input = draw_layer_input(jax.random.fold_in(key_list[4], 71), 0)
    norm_gain = jnp.clip(1.0 + 0.1 * jax.random.normal(key_list[1], (D,), jnp.float32), 0.5, 1.5).astype(jnp.bfloat16)
    kv_weight = centred(key_list[2], (D, 2 * HD), D ** -0.5, 0.09375, ((0, 8),))
    kv_cotangent = centred(key_list[3], (TOKENS, 2 * HD), 4.0, 24.0, ((0, 32),))
    return dict(layer_input=layer_input, norm_gain=norm_gain, kv_weight=kv_weight, kv_cotangent=kv_cotangent)


EPS = 1e-05

def reference(layer_input, norm_gain, kv_weight, kv_cotangent):
    devices = N_INTER * N_INTRA
    gain_wide = norm_gain.astype(jnp.float32)

    def block_step(carry, pieces):
        weight_sum, gain_sum = carry
        rows_in, cotangent = pieces
        widened = rows_in.astype(jnp.float32)
        inverse_rms = lax.rsqrt(lax.optimization_barrier(jnp.mean(widened * widened, axis=1, keepdims=True)) + EPS)
        normal_rows = widened * inverse_rms
        normed = (normal_rows * gain_wide).astype(jnp.bfloat16)
        weight_sum = weight_sum + jnp.dot(normed.T, cotangent, preferred_element_type=jnp.float32)
        feature_grad = jnp.dot(cotangent, kv_weight.T, preferred_element_type=jnp.float32)
        gain_sum = gain_sum + lax.optimization_barrier(jnp.sum(feature_grad * normal_rows, axis=0))
        scaled_grad = feature_grad * gain_wide
        centre = lax.optimization_barrier(jnp.mean(scaled_grad * normal_rows, axis=1, keepdims=True))
        result = (inverse_rms * (scaled_grad - normal_rows * centre)).astype(jnp.bfloat16)
        return ((weight_sum, gain_sum), result)
    blocks_in = layer_input.reshape(devices, TOK_DEV, D)
    blocks_cot = kv_cotangent.reshape(devices, TOK_DEV, 2 * HD)
    start = (jnp.zeros((D, 2 * HD), jnp.float32), jnp.zeros((D,), jnp.float32))
    (weight_sum, gain_sum), grads = lax.scan(block_step, start, (blocks_in, blocks_cot))
    input_grad = grads.reshape(TOKENS, D)
    return (input_grad, weight_sum / float(devices), gain_sum / float(devices))
```

```python
import functools

import jax
import jax.numpy as jnp
from jax import lax
from jax.experimental import pallas as pl
from jax.experimental.pallas import tpu as pltpu
from jax.sharding import PartitionSpec as P

EPS = 1e-05
MESH = pl.DeviceIdType.MESH
LANES = 128


def fused_kernel(m, n, x_hbm, gwin_ref, w_ref, cot_ref, dx_hbm, wg_ref, gg_ref,
                 x_ref, gbuf, gfull, wall, t_ref, pr, xs, xr, u_ref, zs, zr, sref, dxv,
                 x_sem, dx_sem, g_send, g_recv, wz_send, wz_recv, wf_send, wf_recv,
                 p_send, p_recv, x_send, x_recv, z_send, z_recv):
    a, j = lax.axis_index("inter"), lax.axis_index("intra")
    z, c = j // 2, lax.rem(j, 2)
    other = 1 - c
    chips = n // 2
    tokens, features = x_ref.shape
    quarter, pair, shard = features // m, features // chips, features // n
    block = quarter // n
    window = gwin_ref.shape[1]
    low = pair - window

    barrier = pltpu.get_barrier_semaphore()
    for k in range(1, n):
        pl.semaphore_signal(barrier, inc=1, device_id=(a, lax.rem(j + k, n)), device_id_type=MESH)
    for k in range(1, m):
        pl.semaphore_signal(barrier, inc=1, device_id=(lax.rem(a + k, m), j), device_id_type=MESH)
    x_copy = pltpu.make_async_copy(x_hbm, x_ref, x_sem)
    x_copy.start()
    gbuf[j] = gwin_ref[...]
    wall[pl.ds(pl.multiple_of(j * shard, 16), shard), :] = w_ref[...]
    pl.semaphore_wait(barrier, n - 1 + m - 1)

    def send(src, dst, s_sem, r_sem, to):
        copy = pltpu.make_async_remote_copy(src_ref=src, dst_ref=dst, send_sem=s_sem, recv_sem=r_sem,
                                            device_id=to, device_id_type=MESH)
        copy.start()
        return copy

    started = []
    gains = []
    for k in range(1, n):
        gains.append(send(gwin_ref, gbuf.at[j], g_send.at[k - 1], g_recv.at[k - 1], (a, lax.rem(j + k, n))))

    def rows_of(owner):
        return wall.at[pl.ds(pl.multiple_of(owner * shard, 16), shard), :]

    mate = (a, 2 * z + other)
    w_z = []
    for k in range(1, chips):
        to = lax.rem(z + k, chips)
        w_z.append(send(w_ref, rows_of(j), wz_send.at[k - 1], wz_recv.at[k - 1], (a, 2 * to + c)))
    w_f = [send(w_ref, rows_of(j), wf_send.at[0], wf_recv.at[0], mate)]

    x_copy.wait()
    wide = x_ref[...].astype(jnp.float32)
    inv = lax.rsqrt(jnp.mean(wide * wide, axis=1, keepdims=True) + EPS)

    for copy in gains:
        copy.wait_recv()
    for q in range(chips):
        even, odd = gbuf[2 * q], gbuf[2 * q + 1]
        base = q * pair
        gfull[:, base:base + low] = even[:, :low]
        gfull[:, base + low:base + window] = even[:, low:] + odd[:, :window - low]
        gfull[:, base + window:base + pair] = odd[:, window - low:]

    order = list(range(1, m)) + [0]
    p_copies, x_copies = {}, []
    for step in range(m + 1):
        if step < m:
            k = order[step]
            part = lax.rem(a + k, m)
            cols = pl.ds(pl.multiple_of(part * quarter, LANES), quarter)
            normed = (x_ref[:, cols].astype(jnp.float32) * inv * gfull[:, cols]).astype(jnp.bfloat16)
            term = lax.dot_general(normed, cot_ref[...], (((0,), (0,)), ((), ())),
                                   preferred_element_type=jnp.float32)
            for q in range(chips):
                for core in range(2):
                    at = (2 * q + core) * block
                    t_ref[k, core, q * block:(q + 1) * block, :] = term[at:at + block, :]
            p_copies[k] = send(t_ref.at[k, other], pr.at[k], p_send.at[k], p_recv.at[k], mate)
        if step >= 1:
            k = order[step - 1]
            p_copies[k].wait_recv()
            if k:
                xs[k - 1] = (t_ref[k, c] + pr[k]).astype(jnp.bfloat16)
                x_copies.append(send(xs.at[k - 1], xr.at[k - 1], x_send.at[k - 1], x_recv.at[k - 1],
                                     (lax.rem(a + k, m), j)))
            else:
                u_ref[...] = t_ref[0, c] + pr[0]

    for k in range(1, chips):
        w_z[k - 1].wait_recv()
        owner = 2 * lax.rem(z - k + chips, chips) + c
        w_f.append(send(rows_of(owner), rows_of(owner), wf_send.at[k], wf_recv.at[k], mate))

    acc = jnp.zeros((tokens, 1), jnp.float32)

    def feature(k, acc):
        w_f[k].wait_recv()
        q = lax.rem(z - k + chips, chips)
        cols = pl.ds(pl.multiple_of(q * pair, LANES), pair)
        grad = lax.dot_general(cot_ref[...], wall[cols, :], (((1,), (1,)), ((), ())),
                               preferred_element_type=jnp.float32)
        scaled = grad * gfull[:, cols]
        sref[:, cols] = scaled
        normal = x_ref[:, cols].astype(jnp.float32) * inv
        return acc + jnp.sum(scaled * normal, axis=1, keepdims=True)

    for copy in x_copies:
        copy.wait_recv()
    total = u_ref[...]
    for k in range(1, m):
        total = total + xr[k - 1].astype(jnp.float32)
    u_ref[...] = total
    z_copies = []
    for k in range(1, chips):
        to = lax.rem(z + k, chips)
        rows = pl.ds(pl.multiple_of(to * block, 16), block)
        zs[k - 1] = u_ref[rows, :].astype(jnp.bfloat16)
        z_copies.append(send(zs.at[k - 1], zr.at[k - 1], z_send.at[k - 1], z_recv.at[k - 1], (a, 2 * to + c)))

    for k in range(chips):
        acc = feature(k, acc)
    centre = acc * (1.0 / features)
    dx_copies = []
    for q in range(m):
        cols = slice(q * quarter, (q + 1) * quarter)
        normal = x_ref[:, cols].astype(jnp.float32) * inv
        dxv[:, cols] = (inv * (sref[:, cols] - normal * centre)).astype(jnp.bfloat16)
        copy = pltpu.make_async_copy(dxv.at[:, cols], dx_hbm.at[:, cols], dx_sem.at[q])
        copy.start()
        dx_copies.append(copy)

    cols = pl.ds(pl.multiple_of(a * quarter, LANES), quarter)
    lane = lax.broadcasted_iota(jnp.int32, (block, quarter), 1)
    row = lax.broadcasted_iota(jnp.int32, (block, quarter), 0)
    gain = jnp.sum(jnp.where(lane == row + j * block, gfull[:, cols], 0.0), axis=1, keepdims=True)
    own = wall[pl.ds(pl.multiple_of((a * n + j) * block, 16), block), :].astype(jnp.float32) / gain

    for copy in z_copies:
        copy.wait_recv()
    final = u_ref[pl.ds(pl.multiple_of(z * block, 16), block), :]
    for k in range(1, chips):
        final = final + zr[k - 1].astype(jnp.float32)
    final = final / float(m * n)
    wg_ref[...] = final
    ones = jnp.ones((8, final.shape[1]), jnp.float32)
    sums = lax.dot_general(ones, final * own, (((1,), (1,)), ((), ())),
                           precision=lax.Precision.HIGHEST, preferred_element_type=jnp.float32)
    gg_ref[...] = sums[0:1, :]

    for copy in dx_copies:
        copy.wait()
    for copy in gains + w_z + w_f + list(p_copies.values()) + x_copies + z_copies:
        copy.wait_send()


def fused(layer_input, norm_gain, kv_weight, kv_cotangent):
    m, n = lax.axis_size("inter"), lax.axis_size("intra")
    tokens, features = layer_input.shape
    width = kv_weight.shape[1]
    shard = kv_weight.shape[0]
    chips = n // 2
    quarter, pair = features // m, 2 * shard
    block = features // (m * n)
    half = features // m // 2
    window = pair - shard // LANES * LANES
    lead = window - shard
    wide = norm_gain.astype(jnp.float32)
    odd = lax.rem(lax.axis_index("intra"), 2) == 1
    gwin = jnp.where(odd, jnp.pad(wide, (lead, 0)), jnp.pad(wide, (0, lead))).reshape(1, window)
    f32, bf16 = jnp.float32, jnp.bfloat16
    dma = pltpu.SemaphoreType.DMA
    vmem = pl.BlockSpec(memory_space=pltpu.VMEM)
    hbm = pl.BlockSpec(memory_space=pl.ANY)
    dx, wg, gg = pl.pallas_call(
        functools.partial(fused_kernel, m, n),
        out_shape=(
            jax.ShapeDtypeStruct((tokens, features), bf16),
            jax.ShapeDtypeStruct((block, width), f32),
            jax.ShapeDtypeStruct((1, block), f32),
        ),
        in_specs=[hbm, vmem, vmem, vmem],
        out_specs=(hbm, vmem, vmem),
        scratch_shapes=[
            pltpu.VMEM((tokens, features), bf16),
            pltpu.VMEM((n, 1, window), f32),
            pltpu.VMEM((1, features), f32),
            pltpu.VMEM((features, width), bf16),
            pltpu.VMEM((m, 2, half, width), f32),
            pltpu.VMEM((m, half, width), f32),
            pltpu.VMEM((m - 1, half, width), bf16),
            pltpu.VMEM((m - 1, half, width), bf16),
            pltpu.VMEM((half, width), f32),
            pltpu.VMEM((chips - 1, block, width), bf16),
            pltpu.VMEM((chips - 1, block, width), bf16),
            pltpu.VMEM((tokens, features), f32),
            pltpu.VMEM((tokens, features), bf16),
            dma(()), dma((m,)),
            dma((n - 1,)), dma((n - 1,)),
            dma((chips - 1,)), dma((chips - 1,)),
            dma((chips,)), dma((chips,)),
            dma((m,)), dma((m,)),
            dma((m - 1,)), dma((m - 1,)),
            dma((chips - 1,)), dma((chips - 1,)),
        ],
        compiler_params=pltpu.CompilerParams(collective_id=0, has_side_effects=True),
    )(layer_input, gwin, kv_weight, kv_cotangent)
    return dx, wg, gg.reshape(block)


def plain(layer_input, norm_gain, kv_weight, kv_cotangent):
    weight_all, gain_all = (
        lax.all_gather(kv_weight, "intra", axis=0, tiled=True),
        lax.all_gather(norm_gain, "intra", axis=0, tiled=True),
    )
    gain_wide = gain_all.astype(jnp.float32)
    widened = layer_input.astype(jnp.float32)
    inverse_rms = lax.rsqrt(jnp.mean(widened * widened, axis=1, keepdims=True) + EPS)
    normal_rows = widened * inverse_rms
    normed = (normal_rows * gain_wide).astype(jnp.bfloat16)
    weight_term = lax.dot_general(
        normed, kv_cotangent, (((0,), (0,)), ((), ())), preferred_element_type=jnp.float32
    )
    feature_grad = lax.dot_general(
        kv_cotangent, weight_all, (((1,), (1,)), ((), ())), preferred_element_type=jnp.float32
    )
    gain_term = jnp.sum(feature_grad * normal_rows, axis=0)
    outer_count = lax.axis_size("inter")
    inner_count = lax.axis_size("intra")
    devices = outer_count * inner_count
    part_weight, part_gain = (
        lax.psum_scatter(weight_term, "inter", scatter_dimension=0, tiled=True),
        lax.psum_scatter(gain_term, "inter", scatter_dimension=0, tiled=True),
    )
    weight_grad, gain_grad = (
        lax.psum_scatter(part_weight, "intra", scatter_dimension=0, tiled=True),
        lax.psum_scatter(part_gain, "intra", scatter_dimension=0, tiled=True),
    )
    scaled_grad = feature_grad * gain_wide
    centre = jnp.mean(scaled_grad * normal_rows, axis=1, keepdims=True)
    input_grad = (inverse_rms * (scaled_grad - normal_rows * centre)).astype(jnp.bfloat16)
    return (input_grad, weight_grad / float(devices), gain_grad / float(devices))


def on_device(layer_input, norm_gain, kv_weight, kv_cotangent):
    m, n = lax.axis_size("inter"), lax.axis_size("intra")
    features = layer_input.shape[1]
    fits = (
        n % 2 == 0 and n > 2 and m > 1
        and features % (16 * m * n) == 0
        and features % (LANES * m) == 0
        and 2 * features % (LANES * n) == 0
        and layer_input.shape[0] % 16 == 0
        and kv_weight.shape[1] % LANES == 0
    )
    path = fused if fits else plain
    return path(layer_input, norm_gain, kv_weight, kv_cotangent)


def solution(mesh):
    return jax.shard_map(
        on_device,
        mesh=mesh,
        in_specs=(
            P(("inter", "intra"), None),
            P("intra"),
            P("intra", None),
            P(("inter", "intra"), None),
        ),
        out_specs=(P(("inter", "intra"), None), P(("inter", "intra"), None), P(("inter", "intra"))),
        check_vma=False,
    )
```

```python
import functools

import jax
import jax.numpy as jnp
from jax import lax
from jax.experimental import pallas as pl
from jax.experimental.pallas import tpu as pltpu
from jax.sharding import PartitionSpec as P

EPS = 1e-05
MESH = pl.DeviceIdType.MESH
LANES = 128


def fused_kernel(m, n, window, x_hbm, gain_ref, w_ref, cot_ref, dx_ref, wg_ref, gg_ref,
                 x_ref, gwin_ref, gbuf, gfull, wall, t_ref, pr, xs, xr, u_ref, zs, zr, sref,
                 x_sem, g_send, g_recv, wz_send, wz_recv, wf_send, wf_recv,
                 p_send, p_recv, x_send, x_recv, z_send, z_recv):
    a, j = lax.axis_index("inter"), lax.axis_index("intra")
    z, c = j // 2, lax.rem(j, 2)
    other = 1 - c
    chips = n // 2
    tokens, features = x_ref.shape
    quarter, pair, shard = features // m, features // chips, features // n
    block = quarter // n
    low = pair - window

    barrier = pltpu.get_barrier_semaphore()
    for k in range(1, n):
        pl.semaphore_signal(barrier, inc=1, device_id=(a, lax.rem(j + k, n)), device_id_type=MESH)
    for k in range(1, m):
        pl.semaphore_signal(barrier, inc=1, device_id=(lax.rem(a + k, m), j), device_id_type=MESH)
    x_copy = pltpu.make_async_copy(x_hbm, x_ref, x_sem)
    x_copy.start()
    own_gain = gain_ref[...].astype(jnp.float32).reshape(1, shard)
    blank = jnp.zeros((1, window - shard), jnp.float32)
    gwin_ref[...] = jnp.where(c == 1, jnp.concatenate([blank, own_gain], axis=1),
                              jnp.concatenate([own_gain, blank], axis=1))
    gbuf[j] = gwin_ref[...]
    wall[pl.ds(pl.multiple_of(j * shard, 16), shard), :] = w_ref[...]
    x_copy.wait()
    wide = x_ref[...].astype(jnp.float32)
    inv = lax.rsqrt(jnp.mean(wide * wide, axis=1, keepdims=True) + EPS)
    scaled_cot = cot_ref[...].astype(jnp.float32) * inv
    high = scaled_cot.astype(jnp.bfloat16)
    low_half = (scaled_cot - high.astype(jnp.float32)).astype(jnp.bfloat16)
    halves = jnp.concatenate([high, low_half], axis=1)
    width = cot_ref.shape[1]
    pl.semaphore_wait(barrier, n - 1 + m - 1)

    def send(src, dst, s_sem, r_sem, to):
        copy = pltpu.make_async_remote_copy(src_ref=src, dst_ref=dst, send_sem=s_sem, recv_sem=r_sem,
                                            device_id=to, device_id_type=MESH)
        copy.start()
        return copy

    started = []
    gains = []
    for k in range(1, n):
        gains.append(send(gwin_ref, gbuf.at[j], g_send.at[k - 1], g_recv.at[k - 1], (a, lax.rem(j + k, n))))

    def rows_of(owner):
        return wall.at[pl.ds(pl.multiple_of(owner * shard, 16), shard), :]

    mate = (a, 2 * z + other)
    w_z = []
    for k in range(1, chips):
        to = lax.rem(z + k, chips)
        w_z.append(send(w_ref, rows_of(j), wz_send.at[k - 1], wz_recv.at[k - 1], (a, 2 * to + c)))
    w_f = [send(w_ref, rows_of(j), wf_send.at[0], wf_recv.at[0], mate)]

    order = list(range(1, m)) + [0]
    p_copies, x_copies = {}, []
    for step in range(m + 1):
        if step < m:
            k = order[step]
            part = lax.rem(a + k, m)
            cols = pl.ds(pl.multiple_of(part * quarter, LANES), quarter)
            both = lax.dot_general(x_ref[:, cols], halves, (((0,), (0,)), ((), ())),
                                   preferred_element_type=jnp.float32)
            term = both[:, :width] + both[:, width:]
            for q in range(chips):
                for core in range(2):
                    at = (2 * q + core) * block
                    t_ref[k, core, q * block:(q + 1) * block, :] = term[at:at + block, :]
            p_copies[k] = send(t_ref.at[k, other], pr.at[k], p_send.at[k], p_recv.at[k], mate)
        if step >= 1:
            k = order[step - 1]
            p_copies[k].wait_recv()
            if k:
                xs[k - 1] = (t_ref[k, c] + pr[k]).astype(jnp.bfloat16)
                x_copies.append(send(xs.at[k - 1], xr.at[k - 1], x_send.at[k - 1], x_recv.at[k - 1],
                                     (lax.rem(a + k, m), j)))
            else:
                u_ref[...] = t_ref[0, c] + pr[0]

    for copy in gains:
        copy.wait_recv()
    for q in range(chips):
        even, odd = gbuf[2 * q], gbuf[2 * q + 1]
        base = q * pair
        gfull[:, base:base + low] = even[:, :low]
        gfull[:, base + low:base + window] = even[:, low:] + odd[:, :window - low]
        gfull[:, base + window:base + pair] = odd[:, window - low:]

    for k in range(1, chips):
        w_z[k - 1].wait_recv()
        owner = 2 * lax.rem(z - k + chips, chips) + c
        w_f.append(send(rows_of(owner), rows_of(owner), wf_send.at[k], wf_recv.at[k], mate))

    acc = jnp.zeros((tokens, 1), jnp.float32)

    def feature(k, acc):
        w_f[k].wait_recv()
        q = lax.rem(z - k + chips, chips)
        cols = pl.ds(pl.multiple_of(q * pair, LANES), pair)
        grad = lax.dot_general(cot_ref[...], wall[cols, :], (((1,), (1,)), ((), ())),
                               preferred_element_type=jnp.float32)
        scaled = grad * gfull[:, cols]
        sref[:, cols] = scaled
        normal = x_ref[:, cols].astype(jnp.float32) * inv
        return acc + jnp.sum(scaled * normal, axis=1, keepdims=True)

    for copy in x_copies:
        copy.wait_recv()
    total = u_ref[...]
    for k in range(1, m):
        total = total + xr[k - 1].astype(jnp.float32)
    u_ref[...] = total
    z_copies = []
    for k in range(1, chips):
        to = lax.rem(z + k, chips)
        rows = pl.ds(pl.multiple_of(to * block, 16), block)
        zs[k - 1] = u_ref[rows, :].astype(jnp.bfloat16)
        z_copies.append(send(zs.at[k - 1], zr.at[k - 1], z_send.at[k - 1], z_recv.at[k - 1], (a, 2 * to + c)))

    for k in range(chips):
        acc = feature(k, acc)
    centre = acc * (1.0 / features)
    for q in range(m):
        cols = slice(q * quarter, (q + 1) * quarter)
        normal = x_ref[:, cols].astype(jnp.float32) * inv
        dx_ref[:, cols] = (inv * (sref[:, cols] - normal * centre)).astype(jnp.bfloat16)

    cols = pl.ds(pl.multiple_of(a * quarter, LANES), quarter)
    lane = lax.broadcasted_iota(jnp.int32, (block, quarter), 1)
    row = lax.broadcasted_iota(jnp.int32, (block, quarter), 0)
    gain = jnp.sum(jnp.where(lane == row + j * block, gfull[:, cols], 0.0), axis=1, keepdims=True)
    own = wall[pl.ds(pl.multiple_of((a * n + j) * block, 16), block), :].astype(jnp.float32)

    for copy in z_copies:
        copy.wait_recv()
    final = u_ref[pl.ds(pl.multiple_of(z * block, 16), block), :]
    for k in range(1, chips):
        final = final + zr[k - 1].astype(jnp.float32)
    final = final / float(m * n)
    wg_ref[...] = final * gain
    ones = jnp.ones((8, final.shape[1]), jnp.float32)
    sums = lax.dot_general(ones, final * own, (((1,), (1,)), ((), ())),
                           precision=lax.Precision.HIGHEST, preferred_element_type=jnp.float32)
    gg_ref[...] = sums[0:1, :]

    for copy in gains + w_z + w_f + list(p_copies.values()) + x_copies + z_copies:
        copy.wait_send()


def fused(layer_input, norm_gain, kv_weight, kv_cotangent):
    m, n = lax.axis_size("inter"), lax.axis_size("intra")
    tokens, features = layer_input.shape
    width = kv_weight.shape[1]
    shard = kv_weight.shape[0]
    chips = n // 2
    quarter, pair = features // m, 2 * shard
    block = features // (m * n)
    half = features // m // 2
    window = pair - shard // LANES * LANES
    f32, bf16 = jnp.float32, jnp.bfloat16
    dma = pltpu.SemaphoreType.DMA
    vmem = pl.BlockSpec(memory_space=pltpu.VMEM)
    hbm = pl.BlockSpec(memory_space=pltpu.HBM)
    dx, wg, gg = pl.pallas_call(
        functools.partial(fused_kernel, m, n, window),
        out_shape=(
            jax.ShapeDtypeStruct((tokens, features), bf16),
            jax.ShapeDtypeStruct((block, width), f32),
            jax.ShapeDtypeStruct((1, block), f32),
        ),
        in_specs=[hbm, vmem, vmem, vmem],
        out_specs=(vmem, vmem, vmem),
        scratch_shapes=[
            pltpu.VMEM((tokens, features), bf16),
            pltpu.VMEM((1, window), f32),
            pltpu.VMEM((n, 1, window), f32),
            pltpu.VMEM((1, features), f32),
            pltpu.VMEM((features, width), bf16),
            pltpu.VMEM((m, 2, half, width), f32),
            pltpu.VMEM((m, half, width), f32),
            pltpu.VMEM((m - 1, half, width), bf16),
            pltpu.VMEM((m - 1, half, width), bf16),
            pltpu.VMEM((half, width), f32),
            pltpu.VMEM((chips - 1, block, width), bf16),
            pltpu.VMEM((chips - 1, block, width), bf16),
            pltpu.VMEM((tokens, features), f32),
            dma(()),
            dma((n - 1,)), dma((n - 1,)),
            dma((chips - 1,)), dma((chips - 1,)),
            dma((chips,)), dma((chips,)),
            dma((m,)), dma((m,)),
            dma((m - 1,)), dma((m - 1,)),
            dma((chips - 1,)), dma((chips - 1,)),
        ],
        compiler_params=pltpu.CompilerParams(collective_id=0, has_side_effects=True, vmem_limit_bytes=24 * 2**20),
    )(layer_input, norm_gain, kv_weight, kv_cotangent)
    return dx, wg, gg.reshape(block)


def plain(layer_input, norm_gain, kv_weight, kv_cotangent):
    weight_all, gain_all = (
        lax.all_gather(kv_weight, "intra", axis=0, tiled=True),
        lax.all_gather(norm_gain, "intra", axis=0, tiled=True),
    )
    gain_wide = gain_all.astype(jnp.float32)
    widened = layer_input.astype(jnp.float32)
    inverse_rms = lax.rsqrt(jnp.mean(widened * widened, axis=1, keepdims=True) + EPS)
    normal_rows = widened * inverse_rms
    normed = (normal_rows * gain_wide).astype(jnp.bfloat16)
    weight_term = lax.dot_general(
        normed, kv_cotangent, (((0,), (0,)), ((), ())), preferred_element_type=jnp.float32
    )
    feature_grad = lax.dot_general(
        kv_cotangent, weight_all, (((1,), (1,)), ((), ())), preferred_element_type=jnp.float32
    )
    gain_term = jnp.sum(feature_grad * normal_rows, axis=0)
    outer_count = lax.axis_size("inter")
    inner_count = lax.axis_size("intra")
    devices = outer_count * inner_count
    part_weight, part_gain = (
        lax.psum_scatter(weight_term, "inter", scatter_dimension=0, tiled=True),
        lax.psum_scatter(gain_term, "inter", scatter_dimension=0, tiled=True),
    )
    weight_grad, gain_grad = (
        lax.psum_scatter(part_weight, "intra", scatter_dimension=0, tiled=True),
        lax.psum_scatter(part_gain, "intra", scatter_dimension=0, tiled=True),
    )
    scaled_grad = feature_grad * gain_wide
    centre = jnp.mean(scaled_grad * normal_rows, axis=1, keepdims=True)
    input_grad = (inverse_rms * (scaled_grad - normal_rows * centre)).astype(jnp.bfloat16)
    return (input_grad, weight_grad / float(devices), gain_grad / float(devices))


def on_device(layer_input, norm_gain, kv_weight, kv_cotangent):
    m, n = lax.axis_size("inter"), lax.axis_size("intra")
    features = layer_input.shape[1]
    fits = (
        n % 2 == 0 and n > 2 and m > 1
        and features % (16 * m * n) == 0
        and features % (LANES * m) == 0
        and 2 * features % (LANES * n) == 0
        and layer_input.shape[0] % 16 == 0
        and kv_weight.shape[1] % LANES == 0
    )
    path = fused if fits else plain
    return path(layer_input, norm_gain, kv_weight, kv_cotangent)


def solution(mesh):
    return jax.shard_map(
        on_device,
        mesh=mesh,
        in_specs=(
            P(("inter", "intra"), None),
            P("intra"),
            P("intra", None),
            P(("inter", "intra"), None),
        ),
        out_specs=(P(("inter", "intra"), None), P(("inter", "intra"), None), P(("inter", "intra"))),
        check_vma=False,
    )
```

```python
import functools

import jax
import jax.numpy as jnp
from jax import lax
from jax.experimental import pallas as pl
from jax.experimental.pallas import tpu as pltpu
from jax.sharding import PartitionSpec as P

EPS = 1e-05
MESH = pl.DeviceIdType.MESH
LANES = 128
HALVES = 2


def fused_kernel(m, n, window, x_hbm, gain_ref, w_ref, cot_ref, dx_ref, wg_ref, gg_ref,
                 x_ref, gwin_ref, gbuf, gfull, wall, t_ref, pr, xs, xr, u_ref, zs, zr, sref,
                 x_sem, g_send, g_recv, wr_send, wl_send, wz_recv, wf_send, wf_recv,
                 p_send, p_recv, x_send, x_recv, z_send, z_recv):
    a, j = lax.axis_index("inter"), lax.axis_index("intra")
    z, c = j // 2, lax.rem(j, 2)
    other = 1 - c
    chips = n // 2
    tokens, features = x_ref.shape
    quarter, pair, shard = features // m, features // chips, features // n
    block = quarter // n
    low = pair - window

    barrier = pltpu.get_barrier_semaphore()
    for k in range(1, n):
        pl.semaphore_signal(barrier, inc=1, device_id=(a, lax.rem(j + k, n)), device_id_type=MESH)
    for k in range(1, m):
        pl.semaphore_signal(barrier, inc=1, device_id=(lax.rem(a + k, m), j), device_id_type=MESH)
    x_copy = pltpu.make_async_copy(x_hbm, x_ref, x_sem)
    x_copy.start()
    own_gain = gain_ref[...].astype(jnp.float32).reshape(1, shard)
    blank = jnp.zeros((1, window - shard), jnp.float32)
    gwin_ref[...] = jnp.where(c == 1, jnp.concatenate([blank, own_gain], axis=1),
                              jnp.concatenate([own_gain, blank], axis=1))
    gbuf[j] = gwin_ref[...]
    wall[pl.ds(pl.multiple_of(j * shard, 16), shard), :] = w_ref[...]
    x_copy.wait()
    wide = x_ref[...].astype(jnp.float32)
    inv = lax.rsqrt(jnp.mean(wide * wide, axis=1, keepdims=True) + EPS)
    scaled_cot = cot_ref[...].astype(jnp.float32) * inv
    high = scaled_cot.astype(jnp.bfloat16)
    low_half = (scaled_cot - high.astype(jnp.float32)).astype(jnp.bfloat16)
    halves = jnp.concatenate([high, low_half], axis=1)
    width = cot_ref.shape[1]
    pl.semaphore_wait(barrier, n - 1 + m - 1)

    def send(src, dst, s_sem, r_sem, to):
        copy = pltpu.make_async_remote_copy(src_ref=src, dst_ref=dst, send_sem=s_sem, recv_sem=r_sem,
                                            device_id=to, device_id_type=MESH)
        copy.start()
        return copy

    started = []
    gains = []
    for k in range(1, n):
        gains.append(send(gwin_ref, gbuf.at[j], g_send.at[k - 1], g_recv.at[k - 1], (a, lax.rem(j + k, n))))

    piece = shard // HALVES

    def piece_of(chip, core, h):
        return wall.at[pl.ds(pl.multiple_of((2 * chip + core) * shard + h * piece, 16), piece), :]

    mate = (a, 2 * z + other)

    def remote(src, dst, s_sem, r_sem, to):
        return pltpu.make_async_remote_copy(src_ref=src, dst_ref=dst, send_sem=s_sem, recv_sem=r_sem,
                                            device_id=to, device_id_type=MESH)

    def along(chip, h, up, d):
        sems, step = (wr_send, 1) if up else (wl_send, -1)
        to = lax.rem(z + step + chips, chips)
        part = piece_of(chip, c, h)
        src = part if d else w_ref.at[pl.ds(h * piece, piece), :]
        return remote(src, part, sems.at[chip, h], wz_recv.at[chip, h], (a, 2 * to + c))

    def across(chip, h, core, d):
        part = piece_of(chip, core, h)
        src = part if d else w_ref.at[pl.ds(h * piece, piece), :]
        return remote(src, part, wf_send.at[chip, h], wf_recv.at[chip, h], mate)

    def relay(d):
        for h in range(HALVES):
            for up in (True, False):
                chip = z - d if up else z + d

                @pl.when(chip >= 0 if up else chip < chips)
                def _():
                    if d:
                        along(chip, h, up, d).wait_recv()

                    @pl.when(z < chips - 1 if up else z > 0)
                    def _():
                        along(chip, h, up, d).start()

                    if d or up:
                        across(chip, h, c, d).start()

    def settle(d):
        for h in range(HALVES):
            for up in (True, False):
                chip = z - d if up else z + d

                @pl.when(chip >= 0 if up else chip < chips)
                def _():
                    @pl.when(z < chips - 1 if up else z > 0)
                    def _():
                        along(chip, h, up, d).wait_send()

                    if d or up:
                        across(chip, h, c, d).wait_send()

    relay(0)

    order = list(range(1, m)) + [0]
    p_copies, x_copies = {}, []
    for step in range(m + 1):
        if step < m:
            k = order[step]
            part = lax.rem(a + k, m)
            cols = pl.ds(pl.multiple_of(part * quarter, LANES), quarter)
            both = lax.dot_general(x_ref[:, cols], halves, (((0,), (0,)), ((), ())),
                                   preferred_element_type=jnp.float32)
            term = both[:, :width] + both[:, width:]
            for q in range(chips):
                for core in range(2):
                    at = (2 * q + core) * block
                    t_ref[k, core, q * block:(q + 1) * block, :] = term[at:at + block, :]
            p_copies[k] = send(t_ref.at[k, other], pr.at[k], p_send.at[k], p_recv.at[k], mate)
        if step >= 1:
            k = order[step - 1]
            p_copies[k].wait_recv()
            if k:
                xs[k - 1] = (t_ref[k, c] + pr[k]).astype(jnp.bfloat16)
                x_copies.append(send(xs.at[k - 1], xr.at[k - 1], x_send.at[k - 1], x_recv.at[k - 1],
                                     (lax.rem(a + k, m), j)))
            else:
                u_ref[...] = t_ref[0, c] + pr[0]

    for copy in gains:
        copy.wait_recv()
    for q in range(chips):
        even, odd = gbuf[2 * q], gbuf[2 * q + 1]
        base = q * pair
        gfull[:, base:base + low] = even[:, :low]
        gfull[:, base + low:base + window] = even[:, low:] + odd[:, :window - low]
        gfull[:, base + window:base + pair] = odd[:, window - low:]

    relay(1)

    acc = jnp.zeros((tokens, 1), jnp.float32)

    def feature(k, acc):
        q = lax.rem(z + (1 - 2 * (2 * z // chips)) * k + chips, chips)
        for h in range(HALVES):
            across(q, h, other, 1).wait_recv()
        cols = pl.ds(pl.multiple_of(q * pair, LANES), pair)
        grad = lax.dot_general(cot_ref[...], wall[cols, :], (((1,), (1,)), ((), ())),
                               preferred_element_type=jnp.float32)
        scaled = grad * gfull[:, cols]
        sref[:, cols] = scaled
        normal = x_ref[:, cols].astype(jnp.float32) * inv
        return acc + jnp.sum(scaled * normal, axis=1, keepdims=True)

    acc = feature(0, acc)
    for d in range(2, chips - 1):
        relay(d)
    acc = feature(1, acc)

    for copy in x_copies:
        copy.wait_recv()
    total = u_ref[...]
    for k in range(1, m):
        total = total + xr[k - 1].astype(jnp.float32)
    u_ref[...] = total
    z_copies = []
    for k in range(1, chips):
        to = lax.rem(z + k, chips)
        rows = pl.ds(pl.multiple_of(to * block, 16), block)
        zs[k - 1] = u_ref[rows, :].astype(jnp.bfloat16)
        z_copies.append(send(zs.at[k - 1], zr.at[k - 1], z_send.at[k - 1], z_recv.at[k - 1], (a, 2 * to + c)))

    relay(chips - 1)
    for k in range(2, chips):
        acc = feature(k, acc)
    centre = acc * (1.0 / features)
    for q in range(m):
        cols = slice(q * quarter, (q + 1) * quarter)
        normal = x_ref[:, cols].astype(jnp.float32) * inv
        dx_ref[:, cols] = (inv * (sref[:, cols] - normal * centre)).astype(jnp.bfloat16)

    cols = pl.ds(pl.multiple_of(a * quarter, LANES), quarter)
    lane = lax.broadcasted_iota(jnp.int32, (block, quarter), 1)
    row = lax.broadcasted_iota(jnp.int32, (block, quarter), 0)
    gain = jnp.sum(jnp.where(lane == row + j * block, gfull[:, cols], 0.0), axis=1, keepdims=True)
    own = wall[pl.ds(pl.multiple_of((a * n + j) * block, 16), block), :].astype(jnp.float32)

    for copy in z_copies:
        copy.wait_recv()
    final = u_ref[pl.ds(pl.multiple_of(z * block, 16), block), :]
    for k in range(1, chips):
        final = final + zr[k - 1].astype(jnp.float32)
    final = final / float(m * n)
    wg_ref[...] = final * gain
    ones = jnp.ones((8, final.shape[1]), jnp.float32)
    sums = lax.dot_general(ones, final * own, (((1,), (1,)), ((), ())),
                           precision=lax.Precision.HIGHEST, preferred_element_type=jnp.float32)
    gg_ref[...] = sums[0:1, :]

    for copy in gains + list(p_copies.values()) + x_copies + z_copies:
        copy.wait_send()
    for d in range(chips):
        settle(d)


def fused(layer_input, norm_gain, kv_weight, kv_cotangent):
    m, n = lax.axis_size("inter"), lax.axis_size("intra")
    tokens, features = layer_input.shape
    width = kv_weight.shape[1]
    shard = kv_weight.shape[0]
    chips = n // 2
    quarter, pair = features // m, 2 * shard
    block = features // (m * n)
    half = features // m // 2
    window = pair - shard // LANES * LANES
    f32, bf16 = jnp.float32, jnp.bfloat16
    dma = pltpu.SemaphoreType.DMA
    vmem = pl.BlockSpec(memory_space=pltpu.VMEM)
    hbm = pl.BlockSpec(memory_space=pltpu.HBM)
    dx, wg, gg = pl.pallas_call(
        functools.partial(fused_kernel, m, n, window),
        out_shape=(
            jax.ShapeDtypeStruct((tokens, features), bf16),
            jax.ShapeDtypeStruct((block, width), f32),
            jax.ShapeDtypeStruct((1, block), f32),
        ),
        in_specs=[hbm, vmem, vmem, vmem],
        out_specs=(vmem, vmem, vmem),
        scratch_shapes=[
            pltpu.VMEM((tokens, features), bf16),
            pltpu.VMEM((1, window), f32),
            pltpu.VMEM((n, 1, window), f32),
            pltpu.VMEM((1, features), f32),
            pltpu.VMEM((features, width), bf16),
            pltpu.VMEM((m, 2, half, width), f32),
            pltpu.VMEM((m, half, width), f32),
            pltpu.VMEM((m - 1, half, width), bf16),
            pltpu.VMEM((m - 1, half, width), bf16),
            pltpu.VMEM((half, width), f32),
            pltpu.VMEM((chips - 1, block, width), bf16),
            pltpu.VMEM((chips - 1, block, width), bf16),
            pltpu.VMEM((tokens, features), f32),
            dma(()),
            dma((n - 1,)), dma((n - 1,)),
            dma((chips, HALVES)), dma((chips, HALVES)), dma((chips, HALVES)),
            dma((chips, HALVES)), dma((chips, HALVES)),
            dma((m,)), dma((m,)),
            dma((m - 1,)), dma((m - 1,)),
            dma((chips - 1,)), dma((chips - 1,)),
        ],
        compiler_params=pltpu.CompilerParams(collective_id=0, has_side_effects=True, vmem_limit_bytes=24 * 2**20),
    )(*(pltpu.with_memory_space_constraint(v, pltpu.HBM) for v in (layer_input, norm_gain, kv_weight, kv_cotangent)))
    return dx, wg, gg.reshape(block)


def plain(layer_input, norm_gain, kv_weight, kv_cotangent):
    weight_all, gain_all = (
        lax.all_gather(kv_weight, "intra", axis=0, tiled=True),
        lax.all_gather(norm_gain, "intra", axis=0, tiled=True),
    )
    gain_wide = gain_all.astype(jnp.float32)
    widened = layer_input.astype(jnp.float32)
    inverse_rms = lax.rsqrt(jnp.mean(widened * widened, axis=1, keepdims=True) + EPS)
    normal_rows = widened * inverse_rms
    normed = (normal_rows * gain_wide).astype(jnp.bfloat16)
    weight_term = lax.dot_general(
        normed, kv_cotangent, (((0,), (0,)), ((), ())), preferred_element_type=jnp.float32
    )
    feature_grad = lax.dot_general(
        kv_cotangent, weight_all, (((1,), (1,)), ((), ())), preferred_element_type=jnp.float32
    )
    gain_term = jnp.sum(feature_grad * normal_rows, axis=0)
    outer_count = lax.axis_size("inter")
    inner_count = lax.axis_size("intra")
    devices = outer_count * inner_count
    part_weight, part_gain = (
        lax.psum_scatter(weight_term, "inter", scatter_dimension=0, tiled=True),
        lax.psum_scatter(gain_term, "inter", scatter_dimension=0, tiled=True),
    )
    weight_grad, gain_grad = (
        lax.psum_scatter(part_weight, "intra", scatter_dimension=0, tiled=True),
        lax.psum_scatter(part_gain, "intra", scatter_dimension=0, tiled=True),
    )
    scaled_grad = feature_grad * gain_wide
    centre = jnp.mean(scaled_grad * normal_rows, axis=1, keepdims=True)
    input_grad = (inverse_rms * (scaled_grad - normal_rows * centre)).astype(jnp.bfloat16)
    return (input_grad, weight_grad / float(devices), gain_grad / float(devices))


def on_device(layer_input, norm_gain, kv_weight, kv_cotangent):
    m, n = lax.axis_size("inter"), lax.axis_size("intra")
    features = layer_input.shape[1]
    fits = (
        n % 2 == 0 and n > 4 and m > 1
        and kv_weight.shape[0] % (16 * HALVES) == 0
        and features % (16 * m * n) == 0
        and features % (LANES * m) == 0
        and 2 * features % (LANES * n) == 0
        and layer_input.shape[0] % 16 == 0
        and kv_weight.shape[1] % LANES == 0
    )
    path = fused if fits else plain
    return path(layer_input, norm_gain, kv_weight, kv_cotangent)


def solution(mesh):
    return jax.shard_map(
        on_device,
        mesh=mesh,
        in_specs=(
            P(("inter", "intra"), None),
            P("intra"),
            P("intra", None),
            P(("inter", "intra"), None),
        ),
        out_specs=(P(("inter", "intra"), None), P(("inter", "intra"), None), P(("inter", "intra"))),
        check_vma=False,
    )
```

```python
import functools

import jax
import jax.numpy as jnp
from jax import lax
from jax.experimental import pallas as pl
from jax.experimental.pallas import tpu as pltpu
from jax.sharding import PartitionSpec as P

EPS = 1e-05
MESH = pl.DeviceIdType.MESH
LANES = 128
HALVES = 2


def fused_kernel(m, n, window, x_hbm, gain_ref, w_ref, cot_ref, dx_ref, wg_ref, gg_ref,
                 x_ref, gwin_ref, gbuf, gfull, wall, t_ref, pr, xs, xr, u_ref, zs, zr, sref,
                 x_sem, g_send, g_recv, wr_send, wl_send, wz_recv, wf_send, wf_recv,
                 p_send, p_recv, x_send, x_recv, z_send, z_recv):
    a, j = lax.axis_index("inter"), lax.axis_index("intra")
    z, c = j // 2, lax.rem(j, 2)
    other = 1 - c
    chips = n // 2
    tokens, features = x_ref.shape
    quarter, pair, shard = features // m, features // chips, features // n
    block = quarter // n
    low = pair - window

    barrier = pltpu.get_barrier_semaphore()
    for k in range(1, n):
        pl.semaphore_signal(barrier, inc=1, device_id=(a, lax.rem(j + k, n)), device_id_type=MESH)
    for k in range(1, m):
        pl.semaphore_signal(barrier, inc=1, device_id=(lax.rem(a + k, m), j), device_id_type=MESH)
    x_copy = pltpu.make_async_copy(x_hbm, x_ref, x_sem)
    x_copy.start()
    own_gain = gain_ref[...].astype(jnp.float32).reshape(1, shard)
    blank = jnp.zeros((1, window - shard), jnp.float32)
    gwin_ref[...] = jnp.where(c == 1, jnp.concatenate([blank, own_gain], axis=1),
                              jnp.concatenate([own_gain, blank], axis=1))
    gbuf[j] = gwin_ref[...]
    wall[pl.ds(pl.multiple_of(j * shard, 16), shard), :] = w_ref[...]
    x_copy.wait()
    wide = x_ref[...].astype(jnp.float32)
    inv = lax.rsqrt(jnp.mean(wide * wide, axis=1, keepdims=True) + EPS)
    scaled_cot = cot_ref[...].astype(jnp.float32) * inv
    high = scaled_cot.astype(jnp.bfloat16)
    low_half = (scaled_cot - high.astype(jnp.float32)).astype(jnp.bfloat16)
    halves = jnp.concatenate([high, low_half], axis=1)
    width = cot_ref.shape[1]
    pl.semaphore_wait(barrier, n - 1 + m - 1)

    def send(src, dst, s_sem, r_sem, to):
        copy = pltpu.make_async_remote_copy(src_ref=src, dst_ref=dst, send_sem=s_sem, recv_sem=r_sem,
                                            device_id=to, device_id_type=MESH)
        copy.start()
        return copy

    started = []
    gains = []
    for k in range(1, n):
        gains.append(send(gwin_ref, gbuf.at[j], g_send.at[k - 1], g_recv.at[k - 1], (a, lax.rem(j + k, n))))

    piece = shard // HALVES

    def piece_of(chip, core, h):
        return wall.at[pl.ds(pl.multiple_of((2 * chip + core) * shard + h * piece, 16), piece), :]

    mate = (a, 2 * z + other)

    def remote(src, dst, s_sem, r_sem, to):
        return pltpu.make_async_remote_copy(src_ref=src, dst_ref=dst, send_sem=s_sem, recv_sem=r_sem,
                                            device_id=to, device_id_type=MESH)

    def along(chip, h, up, d):
        sems, step = (wr_send, 1) if up else (wl_send, -1)
        to = lax.rem(z + step + chips, chips)
        part = piece_of(chip, c, h)
        src = part if d else w_ref.at[pl.ds(h * piece, piece), :]
        return remote(src, part, sems.at[chip, h], wz_recv.at[chip, h], (a, 2 * to + c))

    def across(chip, h, core, d):
        part = piece_of(chip, core, h)
        src = part if d else w_ref.at[pl.ds(h * piece, piece), :]
        return remote(src, part, wf_send.at[chip, h], wf_recv.at[chip, h], mate)

    def relay(d):
        for h in range(HALVES):
            for up in (True, False):
                chip = z - d if up else z + d

                @pl.when(chip >= 0 if up else chip < chips)
                def _():
                    if d:
                        along(chip, h, up, d).wait_recv()

                    @pl.when(z < chips - 1 if up else z > 0)
                    def _():
                        along(chip, h, up, d).start()

                    if d or up:
                        across(chip, h, c, d).start()

    def settle(d):
        for h in range(HALVES):
            for up in (True, False):
                chip = z - d if up else z + d

                @pl.when(chip >= 0 if up else chip < chips)
                def _():
                    @pl.when(z < chips - 1 if up else z > 0)
                    def _():
                        along(chip, h, up, d).wait_send()

                    if d or up:
                        across(chip, h, c, d).wait_send()

    relay(0)

    order = list(range(1, m)) + [0]
    p_copies, x_copies = {}, []
    for step in range(m + 1):
        if step < m:
            k = order[step]
            part = lax.rem(a + k, m)
            cols = pl.ds(pl.multiple_of(part * quarter, LANES), quarter)
            both = lax.dot_general(x_ref[:, cols], halves, (((0,), (0,)), ((), ())),
                                   preferred_element_type=jnp.float32)
            term = both[:, :width] + both[:, width:]
            for q in range(chips):
                for core in range(2):
                    at = (2 * q + core) * block
                    t_ref[k, core, q * block:(q + 1) * block, :] = term[at:at + block, :]
            p_copies[k] = send(t_ref.at[k, other], pr.at[k], p_send.at[k], p_recv.at[k], mate)
        if step >= 1:
            k = order[step - 1]
            p_copies[k].wait_recv()
            if k:
                xs[k - 1] = (t_ref[k, c] + pr[k]).astype(jnp.bfloat16)
                x_copies.append(send(xs.at[k - 1], xr.at[k - 1], x_send.at[k - 1], x_recv.at[k - 1],
                                     (lax.rem(a + k, m), j)))
            else:
                u_ref[...] = t_ref[0, c] + pr[0]

    for copy in gains:
        copy.wait_recv()
    for q in range(chips):
        even, odd = gbuf[2 * q], gbuf[2 * q + 1]
        base = q * pair
        gfull[:, base:base + low] = even[:, :low]
        gfull[:, base + low:base + window] = even[:, low:] + odd[:, :window - low]
        gfull[:, base + window:base + pair] = odd[:, window - low:]

    relay(1)

    acc = jnp.zeros((tokens, 1), jnp.float32)

    def feature(k, acc):
        q = lax.rem(z + (1 - 2 * (2 * z // chips)) * k + chips, chips)
        for h in range(HALVES):
            across(q, h, other, 1).wait_recv()
        cols = pl.ds(pl.multiple_of(q * pair, LANES), pair)
        grad = lax.dot_general(cot_ref[...], wall[cols, :], (((1,), (1,)), ((), ())),
                               preferred_element_type=jnp.float32)
        scaled = grad * gfull[:, cols]
        sref[:, cols] = scaled
        normal = x_ref[:, cols].astype(jnp.float32) * inv
        return acc + jnp.sum(scaled * normal, axis=1, keepdims=True)

    acc = feature(0, acc)
    for d in range(2, chips - 1):
        relay(d)
    acc = feature(1, acc)

    for copy in x_copies:
        copy.wait_recv()
    total = u_ref[...]
    for k in range(1, m):
        total = total + xr[k - 1].astype(jnp.float32)
    u_ref[...] = total
    z_copies = []
    for k in range(1, chips):
        to = lax.rem(z + k, chips)
        rows = pl.ds(pl.multiple_of(to * block, 16), block)
        zs[k - 1] = u_ref[rows, :].astype(jnp.bfloat16)
        z_copies.append(send(zs.at[k - 1], zr.at[k - 1], z_send.at[k - 1], z_recv.at[k - 1], (a, 2 * to + c)))

    relay(chips - 1)
    for k in range(2, chips):
        acc = feature(k, acc)
    centre = acc * (1.0 / features)
    for q in range(m):
        cols = slice(q * quarter, (q + 1) * quarter)
        normal = x_ref[:, cols].astype(jnp.float32) * inv
        dx_ref[:, cols] = (inv * (sref[:, cols] - normal * centre)).astype(jnp.bfloat16)

    cols = pl.ds(pl.multiple_of(a * quarter, LANES), quarter)
    lane = lax.broadcasted_iota(jnp.int32, (block, quarter), 1)
    row = lax.broadcasted_iota(jnp.int32, (block, quarter), 0)
    gain = jnp.sum(jnp.where(lane == row + j * block, gfull[:, cols], 0.0), axis=1, keepdims=True)
    own = wall[pl.ds(pl.multiple_of((a * n + j) * block, 16), block), :].astype(jnp.float32)

    for copy in z_copies:
        copy.wait_recv()
    final = u_ref[pl.ds(pl.multiple_of(z * block, 16), block), :]
    for k in range(1, chips):
        final = final + zr[k - 1].astype(jnp.float32)
    final = final / float(m * n)
    wg_ref[...] = final * gain
    ones = jnp.ones((8, final.shape[1]), jnp.float32)
    sums = lax.dot_general(ones, final * own, (((1,), (1,)), ((), ())),
                           precision=lax.Precision.HIGHEST, preferred_element_type=jnp.float32)
    gg_ref[...] = sums[0:1, :]

    for copy in gains + list(p_copies.values()) + x_copies + z_copies:
        copy.wait_send()
    for d in range(chips):
        settle(d)


def write_kernel(*refs):
    sources, results, sems = refs[:3], refs[3:6], refs[6]
    copies = [pltpu.make_async_copy(sources[i], results[i], sems.at[i]) for i in range(3)]
    for copy in copies:
        copy.start()
    for copy in copies:
        copy.wait()


def fused(layer_input, norm_gain, kv_weight, kv_cotangent):
    m, n = lax.axis_size("inter"), lax.axis_size("intra")
    tokens, features = layer_input.shape
    width = kv_weight.shape[1]
    shard = kv_weight.shape[0]
    chips = n // 2
    quarter, pair = features // m, 2 * shard
    block = features // (m * n)
    half = features // m // 2
    window = pair - shard // LANES * LANES
    f32, bf16 = jnp.float32, jnp.bfloat16
    dma = pltpu.SemaphoreType.DMA
    vmem = pl.BlockSpec(memory_space=pltpu.VMEM)
    hbm = pl.BlockSpec(memory_space=pltpu.HBM)
    dx, wg, gg = pl.pallas_call(
        functools.partial(fused_kernel, m, n, window),
        out_shape=(
            jax.ShapeDtypeStruct((tokens, features), bf16),
            jax.ShapeDtypeStruct((block, width), f32),
            jax.ShapeDtypeStruct((1, block), f32),
        ),
        in_specs=[hbm, vmem, vmem, vmem],
        out_specs=(vmem, vmem, vmem),
        scratch_shapes=[
            pltpu.VMEM((tokens, features), bf16),
            pltpu.VMEM((1, window), f32),
            pltpu.VMEM((n, 1, window), f32),
            pltpu.VMEM((1, features), f32),
            pltpu.VMEM((features, width), bf16),
            pltpu.VMEM((m, 2, half, width), f32),
            pltpu.VMEM((m, half, width), f32),
            pltpu.VMEM((m - 1, half, width), bf16),
            pltpu.VMEM((m - 1, half, width), bf16),
            pltpu.VMEM((half, width), f32),
            pltpu.VMEM((chips - 1, block, width), bf16),
            pltpu.VMEM((chips - 1, block, width), bf16),
            pltpu.VMEM((tokens, features), f32),
            dma(()),
            dma((n - 1,)), dma((n - 1,)),
            dma((chips, HALVES)), dma((chips, HALVES)), dma((chips, HALVES)),
            dma((chips, HALVES)), dma((chips, HALVES)),
            dma((m,)), dma((m,)),
            dma((m - 1,)), dma((m - 1,)),
            dma((chips - 1,)), dma((chips - 1,)),
        ],
        compiler_params=pltpu.CompilerParams(collective_id=0, has_side_effects=True, vmem_limit_bytes=24 * 2**20),
    )(*(pltpu.with_memory_space_constraint(v, pltpu.HBM) for v in (layer_input, norm_gain, kv_weight, kv_cotangent)))
    dx, wg, gg = pl.pallas_call(
        write_kernel,
        out_shape=tuple(jax.ShapeDtypeStruct(v.shape, v.dtype) for v in (dx, wg, gg)),
        in_specs=[vmem] * 3,
        out_specs=(hbm,) * 3,
        scratch_shapes=[dma((3,))],
        compiler_params=pltpu.CompilerParams(vmem_limit_bytes=8 * 2**20),
    )(dx, wg, gg)
    return dx, wg, gg.reshape(block)


def plain(layer_input, norm_gain, kv_weight, kv_cotangent):
    weight_all, gain_all = (
        lax.all_gather(kv_weight, "intra", axis=0, tiled=True),
        lax.all_gather(norm_gain, "intra", axis=0, tiled=True),
    )
    gain_wide = gain_all.astype(jnp.float32)
    widened = layer_input.astype(jnp.float32)
    inverse_rms = lax.rsqrt(jnp.mean(widened * widened, axis=1, keepdims=True) + EPS)
    normal_rows = widened * inverse_rms
    normed = (normal_rows * gain_wide).astype(jnp.bfloat16)
    weight_term = lax.dot_general(
        normed, kv_cotangent, (((0,), (0,)), ((), ())), preferred_element_type=jnp.float32
    )
    feature_grad = lax.dot_general(
        kv_cotangent, weight_all, (((1,), (1,)), ((), ())), preferred_element_type=jnp.float32
    )
    gain_term = jnp.sum(feature_grad * normal_rows, axis=0)
    outer_count = lax.axis_size("inter")
    inner_count = lax.axis_size("intra")
    devices = outer_count * inner_count
    part_weight, part_gain = (
        lax.psum_scatter(weight_term, "inter", scatter_dimension=0, tiled=True),
        lax.psum_scatter(gain_term, "inter", scatter_dimension=0, tiled=True),
    )
    weight_grad, gain_grad = (
        lax.psum_scatter(part_weight, "intra", scatter_dimension=0, tiled=True),
        lax.psum_scatter(part_gain, "intra", scatter_dimension=0, tiled=True),
    )
    scaled_grad = feature_grad * gain_wide
    centre = jnp.mean(scaled_grad * normal_rows, axis=1, keepdims=True)
    input_grad = (inverse_rms * (scaled_grad - normal_rows * centre)).astype(jnp.bfloat16)
    return (input_grad, weight_grad / float(devices), gain_grad / float(devices))


def on_device(layer_input, norm_gain, kv_weight, kv_cotangent):
    m, n = lax.axis_size("inter"), lax.axis_size("intra")
    features = layer_input.shape[1]
    fits = (
        n % 2 == 0 and n > 4 and m > 1
        and kv_weight.shape[0] % (16 * HALVES) == 0
        and features % (16 * m * n) == 0
        and features % (LANES * m) == 0
        and 2 * features % (LANES * n) == 0
        and layer_input.shape[0] % 16 == 0
        and kv_weight.shape[1] % LANES == 0
    )
    path = fused if fits else plain
    return path(layer_input, norm_gain, kv_weight, kv_cotangent)


def solution(mesh):
    return jax.shard_map(
        on_device,
        mesh=mesh,
        in_specs=(
            P(("inter", "intra"), None),
            P("intra"),
            P("intra", None),
            P(("inter", "intra"), None),
        ),
        out_specs=(P(("inter", "intra"), None), P(("inter", "intra"), None), P(("inter", "intra"))),
        check_vma=False,
    )
```
